32 devices in a mesh: dp: 8 (over y, x, core), tensor: 4 (over z).
Axes of the slice: x: 2, y: 2, z: 4, core: 2. Of those that a mesh axis runs over, the one named last changes fastest.
Arguments:
- tokens: bfloat16 [8192, 1280], P(('dp', 'tensor')), may hold values from -6 to 6
- w_query: bfloat16 [1280, 1280], P('dp', 'tensor'), may hold values from -0.15625 to 0.15625
- w_key: bfloat16 [1280, 1280], P('dp', 'tensor'), may hold values from -0.15625 to 0.15625
- w_value: bfloat16 [1280, 1280], P('dp', 'tensor'), may hold values from -0.15625 to 0.15625
- w_out: bfloat16 [1280, 1280], P('dp', 'tensor'), may hold values from -0.15625 to 0.15625
- w_up: bfloat16 [1280, 5120], P('dp', 'tensor'), may hold values from -0.15625 to 0.15625
- w_gate: bfloat16 [1280, 5120], P('dp', 'tensor'), may hold values from -0.15625 to 0.15625
- w_down: bfloat16 [1280, 5120], P('dp', 'tensor'), may hold values from -0.078125 to 0.078125
- qk_scale: float32 [1280], P('tensor'), may hold values from 0.8 to 1.8
- up_scale: float32 [5120], P('tensor'), may hold values from 0.5 to 2
- gate_scale: float32 [5120], P('tensor'), may hold values from 0.5 to 2
- alpha_attn: float32 [1280], replicated, may hold values from 0.2 to 0.6
- alpha_mlp: float32 [1280], replicated, may hold values from 0.2 to 0.6
- cotangent: bfloat16 [8192, 1280], P(('dp', 'tensor')), may hold values from -6 to 6
Outputs:
- output: bfloat16 [8192, 1280], P(('dp', 'tensor'))
- tokens_gradient: float32 [8192, 1280], P(('dp', 'tensor'))
- w_query_gradient: float32 [1280, 1280], P('dp', 'tensor')
- w_key_gradient: float32 [1280, 1280], P('dp', 'tensor')
- w_value_gradient: float32 [1280, 1280], P('dp', 'tensor')
- w_out_gradient: float32 [1280, 1280], P('dp', 'tensor')
- w_up_gradient: float32 [1280, 5120], P('dp', 'tensor')
- w_gate_gradient: float32 [1280, 5120], P('dp', 'tensor')
- w_down_gradient: float32 [1280, 5120], P('dp', 'tensor')
- qk_scale_gradient: float32 [1280], P('tensor')
- up_scale_gradient: float32 [5120], P('tensor')
- gate_scale_gradient: float32 [5120], P('tensor')
- alpha_attn_gradient: float32 [1280], replicated
- alpha_mlp_gradient: float32 [1280], replicated
The draws below stay inside these ranges and needn't reach their ends.
All inputs are finite; a program needn't handle non-finite values.
Results may differ from the reference program's by a relative error of at most 0.017.
Values may be sent and summed in bfloat16 or wider, within the bound.
A program may use at most 192 MiB of HBM per device.

```python
import math
import jax
import jax.numpy as jnp
from jax import lax

D = 1280
HEADS = 20
HEAD_DIM = 64
FF = 5120
SEQ_LEN = 1024
TOKENS = 8192
N_DP = 8


def shard_levels(own_key, shape, split, low, largest):
    level = 1.0
    for dim, parts in split:
        heights = jax.random.uniform(jax.random.fold_in(jax.random.fold_in(own_key, 6), dim), (parts,), jnp.float32, low / len(split), largest / len(split))
        level = level * jnp.repeat(jnp.exp(heights), shape[dim] // parts).reshape((-1,) + (1,) * (len(shape) - 1 - dim))
    return level


def centred(rng, extent, spread, reach, cuts=(), held_as=jnp.bfloat16):
    array = spread * jax.random.normal(rng, extent, jnp.float32)
    if cuts:
        array = array * shard_levels(rng, extent, cuts, -0.22, 0.18)
    return jnp.clip(array, -reach, reach).astype(held_as)


def setup_inputs(seed: int = 0) -> dict:
    seeds = jax.random.split(jax.random.key(seed), 15)
    return {
        "tokens": centred(seeds[0], (TOKENS, D), 1.0, 6.0, ((0, 32),)),
        "w_query": centred(seeds[1], (D, D), D ** -0.5, 0.15625, ((0, 8), (1, 4))),
        "w_key": centred(seeds[2], (D, D), D ** -0.5, 0.15625, ((0, 8), (1, 4))),
        "w_value": centred(seeds[3], (D, D), D ** -0.5, 0.15625, ((0, 8), (1, 4))),
        "w_out": centred(seeds[4], (D, D), D ** -0.5, 0.15625, ((0, 8), (1, 4))),
        "w_up": centred(seeds[5], (D, FF), D ** -0.5, 0.15625, ((0, 8), (1, 4))),
        "w_gate": centred(seeds[6], (D, FF), D ** -0.5, 0.15625, ((0, 8), (1, 4))),
        "w_down": centred(seeds[7], (D, FF), FF ** -0.5, 0.078125, ((0, 8), (1, 4))),
        "qk_scale": jnp.clip(jnp.exp(math.log(1.8) - 0.8109302 * jax.random.uniform(seeds[8], (D,), jnp.float32) ** shard_levels(seeds[8], (D,), ((0, 4),), -0.2, 0.2)), 0.8, 1.8),
        "up_scale": jnp.clip(jnp.exp(math.log(2.0) - 1.3862944 * jax.random.uniform(seeds[9], (FF,), jnp.float32) ** shard_levels(seeds[9], (FF,), ((0, 4),), -0.2, 0.2)), 0.5, 2.0),
        "gate_scale": jnp.clip(jnp.exp(math.log(2.0) - 1.3862944 * jax.random.uniform(seeds[10], (FF,), jnp.float32) ** shard_levels(seeds[10], (FF,), ((0, 4),), -0.2, 0.2)), 0.5, 2.0),
        "alpha_attn": jnp.clip(jax.random.uniform(seeds[11], (D,), jnp.float32, 0.2, 0.6), 0.2, 0.6),
        "alpha_mlp": jnp.clip(jax.random.uniform(seeds[12], (D,), jnp.float32, 0.2, 0.6), 0.2, 0.6),
        "cotangent": centred(seeds[13], (TOKENS, D), 1.0, 6.0, ((0, 32),)),
    }


HIGH = lax.Precision.HIGHEST
EPS = 1e-06

@jax.custom_vjp
def low(v):
    return lax.optimization_barrier(v.astype(jnp.bfloat16)).astype(jnp.float32)

@jax.custom_vjp
def low_back(v):
    return v

def low_keep(v):
    return (low(v), None)

def low_pass(kept, grad):
    return (grad,)

def back_keep(v):
    return (v, None)

def back_low(kept, grad):
    return (low(grad),)
low.defvjp(low_keep, low_pass)
low_back.defvjp(back_keep, back_low)

def unit_rows(value):
    return value * lax.rsqrt(lax.optimization_barrier(jnp.mean(value * value, axis=-1, keepdims=True)) + EPS)

def matmul(left, right):
    return jnp.dot(left, right, precision=HIGH, preferred_element_type=jnp.float32)

def rotate(value):
    half_dim = HEAD_DIM // 2
    position = jnp.arange(SEQ_LEN, dtype=jnp.float32)[:, None]
    freq_index = jnp.arange(half_dim, dtype=jnp.float32)[None, :]
    frequency = 10000.0 ** (-freq_index / half_dim)
    angle = position * frequency
    cosine = jnp.cos(angle)[:, None, :]
    sine = jnp.sin(angle)[:, None, :]
    first = value[..., :half_dim]
    second = value[..., half_dim:]
    return jnp.concatenate([first * cosine - second * sine, second * cosine + first * sine], axis=-1)

def head_unit(value):
    return value * lax.rsqrt(lax.optimization_barrier(jnp.mean(value * value, axis=-1, keepdims=True)) + EPS)

def layer(seq, wq, wk, wv, wo, wu, wg, wd, sqk, su, sg, alpha_a, alpha_m):
    shape3 = (SEQ_LEN, HEADS, HEAD_DIM)
    scale = HEAD_DIM ** (-0.5)
    q_raw = low_back(matmul(seq, wq)).reshape(shape3)
    k_raw = low_back(matmul(seq, wk)).reshape(shape3)
    values = low(low_back(matmul(seq, wv))).reshape(shape3)
    gains = sqk.reshape(HEADS, HEAD_DIM)
    query = low(head_unit(rotate(q_raw)) * gains)
    keys = low(head_unit(rotate(k_raw)) * gains)
    scores = low_back(jnp.einsum('qhd,khd->hqk', query, keys, precision=HIGH) * scale)
    allowed = jnp.arange(SEQ_LEN)[:, None] >= jnp.arange(SEQ_LEN)[None, :]
    scores = jnp.where(allowed[None], scores, -jnp.inf)
    log_total = jax.nn.logsumexp(scores, axis=-1, keepdims=True)
    probs = low(jnp.exp(scores - log_total))
    attended = jnp.einsum('hqk,khd->qhd', probs, values, precision=HIGH)
    attended = low_back(low(attended)).reshape(SEQ_LEN, D)
    attn_sum = low_back(matmul(attended, wo.T))
    mid = unit_rows(seq + alpha_a * (unit_rows(attn_sum) - seq))
    mid_low = low(mid)
    up_sum = low_back(matmul(mid_low, wu))
    gate_sum = low_back(matmul(mid_low, wg))
    hidden = low(up_sum * su * jax.nn.silu(gate_sum * sg))
    mlp_sum = low_back(matmul(hidden, wd.T))
    return unit_rows(mid + alpha_m * (unit_rows(mlp_sum) - mid))

def reference(tokens, w_query, w_key, w_value, w_out, w_up, w_gate, w_down, qk_scale, up_scale, gate_scale, alpha_attn, alpha_mlp, cotangent):
    floats = tuple((arg.astype(jnp.float32) for arg in (tokens, w_query, w_key, w_value, w_out, w_up, w_gate, w_down, qk_scale, up_scale, gate_scale, alpha_attn, alpha_mlp)))

    def forward(inputs, wq, wk, wv, wo, wu, wg, wd, sqk, su, sg, alpha_a, alpha_m):

        def step(carry, seq):
            return (carry, layer(seq, wq, wk, wv, wo, wu, wg, wd, sqk, su, sg, alpha_a, alpha_m))
        _, finals = lax.scan(jax.checkpoint(step), jnp.zeros((), jnp.float32), inputs.reshape(N_DP, SEQ_LEN, D))
        return finals.reshape(N_DP * SEQ_LEN, D)
    final, pull = jax.vjp(forward, *floats)
    grads = pull(cotangent.astype(jnp.float32))
    return (final.astype(jnp.bfloat16), grads[0], grads[1], grads[2], grads[3], grads[4], grads[5], grads[6], grads[7], grads[8], grads[9], grads[10], grads[11], grads[12])
```

```python
import jax
import jax.numpy as jnp
from jax import lax
from jax.sharding import PartitionSpec as P

HEAD_DIM = 64


HIGH = lax.Precision.HIGHEST
EPS = 1e-06


def unit_rows(value):
    scale = lax.rsqrt(jnp.mean(value * value, axis=-1, keepdims=True) + EPS)
    return (value * scale, scale)


def unit_back(grad, unit, scale):
    return scale * (grad - unit * jnp.mean(grad * unit, axis=-1, keepdims=True))


def contract_rows(left, right):
    return lax.dot_general(
        left, right, (((0,), (0,)), ((), ())), preferred_element_type=jnp.float32
    )


def contract_cols(left, right):
    return lax.dot_general(
        left, right, (((1,), (1,)), ((), ())), preferred_element_type=jnp.float32
    )


def tables(width, length):
    half_dim = HEAD_DIM // 2
    column = lax.iota(jnp.int32, width)
    within = column % HEAD_DIM
    freq_index = (within % half_dim).astype(jnp.float32)
    frequency = 10000.0 ** (-freq_index / half_dim)
    position = lax.iota(jnp.float32, length)
    angle = position[:, None] * frequency[None, :]
    first_half = (within < half_dim)[None, :]
    heads = width // HEAD_DIM
    member = (
        lax.broadcasted_iota(jnp.int32, (width, heads), 0) // HEAD_DIM
        == lax.broadcasted_iota(jnp.int32, (width, heads), 1)
    ).astype(jnp.float32)
    return (jnp.cos(angle), jnp.sin(angle), first_half, member)


def rope_apply(value, cosine, sine, first_half):
    half_dim = HEAD_DIM // 2
    turned = jnp.where(
        first_half, -jnp.roll(value, -half_dim, axis=1), jnp.roll(value, half_dim, axis=1)
    )
    return value * cosine + turned * sine


def rope_back(grad, cosine, sine, first_half):
    half_dim = HEAD_DIM // 2
    weighted = grad * sine
    turned = jnp.where(
        first_half, jnp.roll(weighted, -half_dim, axis=1), -jnp.roll(weighted, half_dim, axis=1)
    )
    return grad * cosine + turned


def head_unit(value, member):
    mean_sq = (
        jnp.dot(value * value, member, precision=HIGH, preferred_element_type=jnp.float32)
        / HEAD_DIM
    )
    scale = jnp.dot(
        lax.rsqrt(mean_sq + EPS), member.T, precision=HIGH, preferred_element_type=jnp.float32
    )
    return (value * scale, scale)


def head_back(grad, unit, scale, member):
    inner = (
        jnp.dot(grad * unit, member, precision=HIGH, preferred_element_type=jnp.float32) / HEAD_DIM
    )
    spread = jnp.dot(inner, member.T, precision=HIGH, preferred_element_type=jnp.float32)
    return scale * (grad - unit * spread)


def block_scores(query3, key3, start, stop, block):
    scale = HEAD_DIM ** (-0.5)
    scores = (
        jnp.einsum(
            "qhd,khd->hqk", query3[start:stop], key3[:stop], preferred_element_type=jnp.float32
        )
        * scale
    )
    allowed = start + lax.broadcasted_iota(jnp.int32, (block, stop), 0) >= lax.broadcasted_iota(
        jnp.int32, (block, stop), 1
    )
    return jnp.where(allowed[None], scores, -jnp.inf)


def attend(query3, key3, value3, block):
    length = query3.shape[0]
    outputs = []
    totals = []
    for block_id in range(length // block):
        start = block_id * block
        stop = start + block
        scores = block_scores(query3, key3, start, stop, block)
        row_max = jnp.max(scores, axis=-1, keepdims=True)
        log_total = jnp.log(jnp.sum(jnp.exp(scores - row_max), axis=-1, keepdims=True)) + row_max
        weights = jnp.exp(scores - log_total).astype(jnp.bfloat16)
        outputs.append(
            jnp.einsum("hqk,khd->qhd", weights, value3[:stop], preferred_element_type=jnp.float32)
        )
        totals.append(log_total)
    return (jnp.concatenate(outputs, axis=0), totals)


def attend_back(query3, key3, value3, grad3, totals, block):
    length = query3.shape[0]
    scale = HEAD_DIM ** (-0.5)
    query_parts = []
    key_grad = jnp.zeros(key3.shape, jnp.float32)
    value_grad = jnp.zeros(value3.shape, jnp.float32)
    for block_id in range(length // block):
        start = block_id * block
        stop = start + block
        scores = block_scores(query3, key3, start, stop, block)
        probs = jnp.exp(scores - totals[block_id])
        g_probs = jnp.einsum(
            "qhd,khd->hqk", grad3[start:stop], value3[:stop], preferred_element_type=jnp.float32
        )
        inner = jnp.sum(probs * g_probs, axis=-1, keepdims=True)
        g_scores = (probs * (g_probs - inner)).astype(jnp.bfloat16)
        query_parts.append(
            jnp.einsum("hqk,khd->qhd", g_scores, key3[:stop], preferred_element_type=jnp.float32)
            * scale
        )
        key_grad = key_grad.at[:stop].add(
            jnp.einsum(
                "hqk,qhd->khd", g_scores, query3[start:stop], preferred_element_type=jnp.float32
            )
            * scale
        )
        value_grad = value_grad.at[:stop].add(
            jnp.einsum(
                "hqk,qhd->khd",
                probs.astype(jnp.bfloat16),
                grad3[start:stop],
                preferred_element_type=jnp.float32,
            )
        )
    return (jnp.concatenate(query_parts, axis=0), key_grad, value_grad)


def scatter_low(value, axis):
    return lax.psum_scatter(
        value.astype(jnp.bfloat16), axis, scatter_dimension=0, tiled=True
    ).astype(jnp.float32)


def on_device(
    tokens,
    w_query,
    w_key,
    w_value,
    w_out,
    w_up,
    w_gate,
    w_down,
    qk_scale,
    up_scale,
    gate_scale,
    alpha_attn,
    alpha_mlp,
    cotangent,
):
    attn_w = lax.all_gather(
        jnp.concatenate([w_query, w_key, w_value, w_out], axis=1), "dp", axis=0, tiled=True
    )
    query_w, key_w, value_w, out_w = jnp.split(attn_w, 4, axis=1)
    whole = lax.all_gather(tokens, "tensor", axis=0, tiled=True)
    mlp_w = lax.all_gather(
        jnp.concatenate([w_up, w_gate, w_down], axis=1), "dp", axis=0, tiled=True
    )
    up_w, gate_w, down_w = jnp.split(mlp_w, 3, axis=1)
    length = whole.shape[0]
    width = query_w.shape[1]
    block = min(512, length)
    cosine, sine, first_half, member = tables(width, length)
    shape3 = (length, width // HEAD_DIM, HEAD_DIM)
    q_raw = jnp.dot(whole, query_w, preferred_element_type=jnp.float32)
    k_raw = jnp.dot(whole, key_w, preferred_element_type=jnp.float32)
    value_low = jnp.dot(whole, value_w, preferred_element_type=jnp.float32).astype(jnp.bfloat16)
    q_unit, q_norm = head_unit(rope_apply(q_raw, cosine, sine, first_half), member)
    k_unit, k_norm = head_unit(rope_apply(k_raw, cosine, sine, first_half), member)
    query_low = (q_unit * qk_scale).astype(jnp.bfloat16)
    key_low = (k_unit * qk_scale).astype(jnp.bfloat16)
    query3 = query_low.reshape(shape3)
    key3 = key_low.reshape(shape3)
    value3 = value_low.reshape(shape3)
    attended, totals = attend(query3, key3, value3, block)
    attended_low = attended.reshape(length, width).astype(jnp.bfloat16)
    attn_sum = scatter_low(contract_cols(attended_low, out_w), "tensor")
    attn_unit, attn_norm = unit_rows(attn_sum)
    residual = tokens.astype(jnp.float32)
    mid, mid_norm = unit_rows(residual + alpha_attn * (attn_unit - residual))
    mid_low = mid.astype(jnp.bfloat16)
    mid_whole = lax.all_gather(mid_low, "tensor", axis=0, tiled=True)
    up_sum = jnp.dot(mid_whole, up_w, preferred_element_type=jnp.float32)
    gate_sum = jnp.dot(mid_whole, gate_w, preferred_element_type=jnp.float32)
    up_val = up_sum * up_scale
    gate_val = gate_sum * gate_scale
    sigma = jax.nn.sigmoid(gate_val)
    hidden_low = (up_val * (gate_val * sigma)).astype(jnp.bfloat16)
    mlp_sum = scatter_low(contract_cols(hidden_low, down_w), "tensor")
    mlp_unit, mlp_norm = unit_rows(mlp_sum)
    final, final_norm = unit_rows(mid + alpha_mlp * (mlp_unit - mid))
    output = final.astype(jnp.bfloat16)
    g_second = unit_back(cotangent.astype(jnp.float32), final, final_norm)
    g_alpha_mlp = jnp.sum((mlp_unit - mid) * g_second, axis=0)
    g_mlp_low = unit_back(alpha_mlp * g_second, mlp_unit, mlp_norm).astype(jnp.bfloat16)
    g_mlp_whole = lax.all_gather(g_mlp_low, "tensor", axis=0, tiled=True)
    down_grad = contract_rows(g_mlp_whole, hidden_low)
    g_hidden = jnp.dot(g_mlp_whole, down_w, preferred_element_type=jnp.float32)
    g_up = g_hidden * (gate_val * sigma)
    g_gate = g_hidden * up_val * (sigma * (1.0 + gate_val * (1.0 - sigma)))
    up_scale_grad = jnp.sum(g_up * up_sum, axis=0)
    gate_scale_grad = jnp.sum(g_gate * gate_sum, axis=0)
    g_up_low = (g_up * up_scale).astype(jnp.bfloat16)
    g_gate_low = (g_gate * gate_scale).astype(jnp.bfloat16)
    up_grad = contract_rows(mid_whole, g_up_low)
    gate_grad = contract_rows(mid_whole, g_gate_low)
    g_mid_part = contract_cols(g_up_low, up_w) + contract_cols(g_gate_low, gate_w)
    g_mid = (1.0 - alpha_mlp) * g_second + scatter_low(g_mid_part, "tensor")
    up_grad, gate_grad, down_grad = jnp.split(
        scatter_low(jnp.concatenate([up_grad, gate_grad, down_grad], axis=1), "dp"), 3, axis=1
    )
    g_first = unit_back(g_mid, mid, mid_norm)
    g_alpha_attn = jnp.sum((attn_unit - residual) * g_first, axis=0)
    g_attn_low = unit_back(alpha_attn * g_first, attn_unit, attn_norm).astype(jnp.bfloat16)
    g_attn_whole = lax.all_gather(g_attn_low, "tensor", axis=0, tiled=True)
    out_grad = contract_rows(g_attn_whole, attended_low)
    g_attended_low = jnp.dot(g_attn_whole, out_w, preferred_element_type=jnp.float32).astype(
        jnp.bfloat16
    )
    g_query3, g_key3, g_value3 = attend_back(
        query3, key3, value3, g_attended_low.reshape(shape3), totals, block
    )
    g_query = g_query3.reshape(length, width)
    g_key = g_key3.reshape(length, width)
    qk_grad = jnp.sum(g_query * q_unit, axis=0) + jnp.sum(g_key * k_unit, axis=0)
    g_q_raw_low = rope_back(
        head_back(g_query * qk_scale, q_unit, q_norm, member), cosine, sine, first_half
    ).astype(jnp.bfloat16)
    g_k_raw_low = rope_back(
        head_back(g_key * qk_scale, k_unit, k_norm, member), cosine, sine, first_half
    ).astype(jnp.bfloat16)
    g_value_low = g_value3.reshape(length, width).astype(jnp.bfloat16)
    query_grad = contract_rows(whole, g_q_raw_low)
    key_grad = contract_rows(whole, g_k_raw_low)
    value_grad = contract_rows(whole, g_value_low)
    g_tok_part = (
        contract_cols(g_q_raw_low, query_w)
        + contract_cols(g_k_raw_low, key_w)
        + contract_cols(g_value_low, value_w)
    )
    tokens_grad = (1.0 - alpha_attn) * g_first + lax.psum_scatter(
        g_tok_part.astype(jnp.bfloat16), "tensor", scatter_dimension=0, tiled=True
    ).astype(jnp.float32)
    query_grad, key_grad, value_grad, out_grad = jnp.split(
        scatter_low(
            jnp.concatenate([query_grad, key_grad, value_grad, out_grad], axis=1), "dp"
        ),
        4,
        axis=1,
    )
    sizes = (g_alpha_attn.shape[0], g_alpha_mlp.shape[0], up_scale_grad.shape[0], gate_scale_grad.shape[0])
    cuts = (sizes[0], sizes[0] + sizes[1], sum(sizes[:3]), sum(sizes))
    small = jnp.sum(
        lax.all_gather(
            jnp.concatenate([g_alpha_attn, g_alpha_mlp, up_scale_grad, gate_scale_grad, qk_grad]),
            "dp",
        ),
        axis=0,
    )
    alphas = jnp.sum(lax.all_gather(small[: cuts[1]], "tensor"), axis=0)
    g_alpha_attn, g_alpha_mlp = alphas[: cuts[0]], alphas[cuts[0] :]
    up_scale_grad = small[cuts[1] : cuts[2]]
    gate_scale_grad = small[cuts[2] : cuts[3]]
    qk_grad = small[cuts[3] :]
    return (
        output,
        tokens_grad,
        query_grad,
        key_grad,
        value_grad,
        out_grad,
        up_grad,
        gate_grad,
        down_grad,
        qk_grad,
        up_scale_grad,
        gate_scale_grad,
        g_alpha_attn,
        g_alpha_mlp,
    )


def solution(mesh):
    in_specs = (
        P(("dp", "tensor"), None),
        P("dp", "tensor"),
        P("dp", "tensor"),
        P("dp", "tensor"),
        P("dp", "tensor"),
        P("dp", "tensor"),
        P("dp", "tensor"),
        P("dp", "tensor"),
        P("tensor"),
        P("tensor"),
        P("tensor"),
        P(),
        P(),
        P(("dp", "tensor"), None),
    )
    out_specs = (
        P(("dp", "tensor"), None),
        P(("dp", "tensor"), None),
        P("dp", "tensor"),
        P("dp", "tensor"),
        P("dp", "tensor"),
        P("dp", "tensor"),
        P("dp", "tensor"),
        P("dp", "tensor"),
        P("dp", "tensor"),
        P("tensor"),
        P("tensor"),
        P("tensor"),
        P(),
        P(),
    )
    return jax.shard_map(
        on_device, mesh=mesh, in_specs=in_specs, out_specs=out_specs, check_vma=False
    )
```

```python
import functools

import jax
import jax.numpy as jnp
from jax import lax
from jax.experimental import pallas as pl
from jax.experimental.pallas import tpu as pltpu
from jax.sharding import PartitionSpec as P

HEAD_DIM = 64


HIGH = lax.Precision.HIGHEST
EPS = 1e-06


MESH_ID = pl.DeviceIdType.MESH
ANY = pl.BlockSpec(memory_space=pl.ANY)
IN_VMEM = pl.BlockSpec(memory_space=pltpu.VMEM)


def remote(src, dst, send, recv, target):
    return pltpu.make_async_remote_copy(
        src_ref=src, dst_ref=dst, send_sem=send, recv_sem=recv,
        device_id=target, device_id_type=MESH_ID,
    )


def meet(partners):
    barrier = pltpu.get_barrier_semaphore()
    count = 0
    for there, target in partners:
        if there is True:
            pl.semaphore_signal(barrier, inc=1, device_id=target, device_id_type=MESH_ID)
            count = count + 1
        else:
            @pl.when(there)
            def _():
                pl.semaphore_signal(barrier, inc=1, device_id=target, device_id_type=MESH_ID)
            count = count + there.astype(jnp.int32)
    pl.semaphore_wait(barrier, count)


def line_partners(me, count):
    return [
        (me < count - 1, {"tensor": jnp.minimum(me + 1, count - 1)}),
        (me > 0, {"tensor": jnp.maximum(me - 1, 0)}),
    ]


def plane_partners():
    dp = lax.axis_index("dp")
    return [(True, {"dp": dp + bit * (1 - 2 * ((dp // bit) % 2))}) for bit in (1, 2, 4)]


class LineGather:
    def __init__(self, own, out, send, recv, count, pieces):
        self.own, self.out, self.send, self.recv = own, out, send, recv
        self.count, self.pieces = count, pieces
        self.me = lax.axis_index("tensor")
        self.rows = own.shape[0] // pieces

    def hop(self, way, origin, piece, step):
        target = {"tensor": self.me + way}
        place = self.out.at[origin, pl.ds(piece * self.rows, self.rows)]
        src = self.own.at[pl.ds(piece * self.rows, self.rows)] if step == 0 else place
        side = 0 if way == 1 else 1
        return remote(
            src, place, self.send.at[side, step, piece], self.recv.at[side, step, piece], target
        )

    def can_send(self, way, step):
        near = self.me + way
        origin = self.me - way * step
        return (near >= 0) & (near < self.count) & (origin >= 0) & (origin < self.count)

    def start(self, step, piece):
        for way in (1, -1):
            @pl.when(self.can_send(way, step))
            def _():
                self.hop(way, self.me - way * step, piece, step).start()

    def arrive(self, step, piece):
        for way in (1, -1):
            origin = self.me - way * (step + 1)
            @pl.when((origin >= 0) & (origin < self.count))
            def _():
                place = self.out.at[origin, pl.ds(piece * self.rows, self.rows)]
                side = 0 if way == 1 else 1
                remote(
                    place, place, self.send.at[side, step, piece],
                    self.recv.at[side, step, piece], {"tensor": self.me - way},
                ).wait_recv()

    def finish(self):
        for step in range(self.count - 1):
            for piece in range(self.pieces):
                for way in (1, -1):
                    @pl.when(self.can_send(way, step))
                    def _():
                        self.hop(way, self.me - way * step, piece, step).wait_send()


def gather_kernel(
    count, pieces, tokens, shard, whole, full, line_send, line_recv, send, recv, local
):
    dp = lax.axis_index("dp")
    flip = [dp + bit * (1 - 2 * ((dp // bit) % 2)) for bit in (1, 2, 4)]
    core, near_x, near_y = flip
    far = near_x + 4 * (1 - 2 * ((dp // 4) % 2))
    half = shard.shape[0] // 2
    meet(line_partners(lax.axis_index("tensor"), count) + plane_partners())
    line = LineGather(tokens, whole, line_send, line_recv, count, pieces)

    def part(origin, which):
        return full.at[origin, pl.ds(which * half, half)]

    def flow(slot, src, origin, which, target):
        return remote(src, part(origin, which), send.at[slot], recv.at[slot], {"dp": target})

    mine = [shard.at[pl.ds(which * half, half)] for which in (0, 1)]
    for piece in range(pieces):
        line.start(0, piece)
    started = []

    def go(slot, src, origin, which, target):
        copy = flow(slot, src, origin, which, target)
        copy.start()
        started.append(copy)

    def got(slot, origin, which):
        place = part(origin, which)
        remote(place, place, send.at[slot], recv.at[slot], {"dp": core}).wait_recv()

    go(0, mine[0], dp, 0, near_x)
    go(2, mine[1], dp, 1, near_y)
    go(1, mine[1], dp, 1, near_x)
    go(3, mine[0], dp, 0, near_y)
    go(6, mine[0], dp, 0, core)
    go(7, mine[1], dp, 1, core)
    keep = [
        pltpu.make_async_copy(shard, full.at[dp], local.at[0]),
        pltpu.make_async_copy(tokens, whole.at[line.me], local.at[1]),
    ]
    for copy in keep:
        copy.start()
    for piece in range(pieces):
        line.arrive(0, piece)
        line.start(1, piece)
    got(0, near_x, 0)
    go(4, part(near_x, 0), near_x, 0, near_y)
    go(8, part(near_x, 0), near_x, 0, core)
    got(2, near_y, 1)
    go(5, part(near_y, 1), near_y, 1, near_x)
    go(9, part(near_y, 1), near_y, 1, core)
    for step in range(1, count - 1):
        for piece in range(pieces):
            line.arrive(step, piece)
            if step + 1 < count - 1:
                line.start(step + 1, piece)
    got(1, near_x, 1)
    go(10, part(near_x, 1), near_x, 1, core)
    got(3, near_y, 0)
    go(11, part(near_y, 0), near_y, 0, core)
    got(4, far, 0)
    go(12, part(far, 0), far, 0, core)
    got(5, far, 1)
    go(13, part(far, 1), far, 1, core)
    def other(index):
        return index + 1 - 2 * (index % 2)
    for slot, origin, which in (
        (6, core, 0), (7, core, 1), (8, other(near_x), 0), (9, other(near_y), 1),
        (10, other(near_x), 1), (11, other(near_y), 0), (12, other(far), 0), (13, other(far), 1),
    ):
        got(slot, origin, which)
    for copy in started:
        copy.wait_send()
    line.finish()
    for copy in keep:
        copy.wait()


def gather_all(tokens, shard, count, size, pieces=2):
    return pl.pallas_call(
        functools.partial(gather_kernel, count, pieces),
        out_shape=(
            jax.ShapeDtypeStruct((count,) + tokens.shape, tokens.dtype),
            jax.ShapeDtypeStruct((size,) + shard.shape, shard.dtype),
        ),
        in_specs=[IN_VMEM, IN_VMEM],
        out_specs=(ANY, ANY),
        scratch_shapes=[
            pltpu.SemaphoreType.DMA((2, count - 1, pieces)),
            pltpu.SemaphoreType.DMA((2, count - 1, pieces)),
            pltpu.SemaphoreType.DMA((14,)),
            pltpu.SemaphoreType.DMA((14,)),
            pltpu.SemaphoreType.DMA((2,)),
        ],
        compiler_params=pltpu.CompilerParams(collective_id=1, has_side_effects=True),
        name="gather_all",
    )(tokens, shard)


def everyone(count, size):
    me, dp = lax.axis_index("tensor"), lax.axis_index("dp")
    return [(True, {"tensor": lax.rem(me + k, count)}) for k in range(1, count)] + [
        (True, {"dp": lax.rem(dp + k, size)}) for k in range(1, size)
    ]


def add_rows(dst, left, right, rows):
    step = 16
    def body(index, carry):
        at = pl.ds(pl.multiple_of(index * step, step), step)
        total = left[at, :].astype(jnp.float32) + right[at, :].astype(jnp.float32)
        dst[at, :] = total.astype(dst.dtype)
        return carry
    lax.fori_loop(0, rows // step, body, 0)


class LineScatter:
    def __init__(self, parts, inbox, outbox, send, recv, count, pieces):
        self.parts, self.inbox, self.outbox = parts, inbox, outbox
        self.send, self.recv = send, recv
        self.count, self.pieces = count, pieces
        self.me = lax.axis_index("tensor")
        self.rows = parts.shape[1] // pieces

    def at(self, piece):
        return pl.ds(piece * self.rows, self.rows)

    def copy(self, way, src, dest, piece):
        side = 0 if way == 1 else 1
        return remote(
            src, self.inbox.at[side, dest, self.at(piece)],
            self.send.at[side, dest, piece], self.recv.at[side, dest, piece],
            {"tensor": self.me + way},
        )

    def hops(self, way):
        return self.me if way == 1 else self.count - 1 - self.me

    def begin(self):
        for turn in range(self.count - 1):
            for piece in range(self.pieces):
                for way in (1, -1):
                    dest = self.count - 1 - turn if way == 1 else turn
                    @pl.when(self.hops(way) == 0)
                    def _():
                        self.copy(way, self.parts.at[dest, self.at(piece)], dest, piece).start()

    def relay(self, time, piece):
        for way in (1, -1):
            side = 0 if way == 1 else 1
            turn = time - self.hops(way)
            dest = self.count - 1 - turn if way == 1 else turn
            beyond = dest > self.me if way == 1 else dest < self.me
            @pl.when((self.hops(way) > 0) & (turn >= 0) & beyond)
            def _():
                rows = self.at(piece)
                src = self.outbox.at[side, dest, rows]
                self.copy(way, src, dest, piece).wait_recv()
                add_rows(
                    src, self.parts.at[dest, rows], self.inbox.at[side, dest, rows], self.rows
                )
                self.copy(way, src, dest, piece).start()

    def take(self, total):
        step = 16
        def first(index, carry):
            at = pl.ds(pl.multiple_of(index * step, step), step)
            total[at, :] = self.parts[self.me, at, :].astype(jnp.float32)
            return carry
        lax.fori_loop(0, self.parts.shape[1] // step, first, 0)
        for piece in range(self.pieces):
            for way in (1, -1):
                side = 0 if way == 1 else 1
                @pl.when(self.hops(way) > 0)
                def _():
                    rows = self.at(piece)
                    self.copy(way, self.inbox.at[side, self.me, rows], self.me, piece).wait_recv()
                    add_rows(
                        total.at[rows], total.at[rows], self.inbox.at[side, self.me, rows],
                        self.rows,
                    )

    def finish(self):
        for turn in range(self.count - 1):
            for piece in range(self.pieces):
                for way in (1, -1):
                    dest = self.count - 1 - turn if way == 1 else turn
                    sent = dest > self.me if way == 1 else dest < self.me
                    @pl.when(sent)
                    def _():
                        self.copy(
                            way, self.outbox.at[0 if way == 1 else 1, dest, self.at(piece)],
                            dest, piece,
                        ).wait_send()


def line_boxes(count, rows, cols, pieces):
    return [
        pltpu.VMEM((2, count, rows, cols), jnp.bfloat16),
        pltpu.VMEM((2, count, rows, cols), jnp.bfloat16),
        pltpu.SemaphoreType.DMA((2, count, pieces)),
        pltpu.SemaphoreType.DMA((2, count, pieces)),
    ]


def line_gather_kernel(count, pieces, own, whole, send, recv, local):
    meet(line_partners(lax.axis_index("tensor"), count))
    line = LineGather(own, whole, send, recv, count, pieces)
    for piece in range(pieces):
        line.start(0, piece)
    keep = pltpu.make_async_copy(own, whole.at[line.me], local.at[0])
    keep.start()
    for step in range(count - 1):
        for piece in range(pieces):
            line.arrive(step, piece)
            if step + 1 < count - 1:
                line.start(step + 1, piece)
    line.finish()
    keep.wait()


def line_gather(own, count, ident, pieces=4):
    return pl.pallas_call(
        functools.partial(line_gather_kernel, count, pieces),
        out_shape=jax.ShapeDtypeStruct((count,) + own.shape, own.dtype),
        in_specs=[IN_VMEM],
        out_specs=IN_VMEM,
        scratch_shapes=[
            pltpu.SemaphoreType.DMA((2, count - 1, pieces)),
            pltpu.SemaphoreType.DMA((2, count - 1, pieces)),
            pltpu.SemaphoreType.DMA((1,)),
        ],
        compiler_params=pltpu.CompilerParams(collective_id=ident, has_side_effects=True),
        name=f"line_gather_{ident}",
    )(own).reshape(count * own.shape[0], own.shape[1])


def line_scatter_kernel(count, pieces, parts, total, inbox, outbox, send, recv):
    meet(line_partners(lax.axis_index("tensor"), count))
    line = LineScatter(parts, inbox, outbox, send, recv, count, pieces)
    line.begin()
    for time in range(1, count - 1):
        for piece in range(pieces):
            line.relay(time, piece)
    line.take(total)
    line.finish()


def line_scatter(value, count, ident, pieces=4):
    rows, cols = value.shape[0] // count, value.shape[1]
    return pl.pallas_call(
        functools.partial(line_scatter_kernel, count, pieces),
        out_shape=jax.ShapeDtypeStruct((rows, cols), jnp.float32),
        in_specs=[IN_VMEM],
        out_specs=IN_VMEM,
        scratch_shapes=line_boxes(count, rows, cols, pieces),
        compiler_params=pltpu.CompilerParams(collective_id=ident, has_side_effects=True),
        name=f"line_scatter_{ident}",
    )(value.astype(jnp.bfloat16).reshape(count, rows, cols))


def scatter_kernel(
    count, size, pieces, parts, grads, small, total, mine, summed,
    inbox, outbox, line_send, line_recv,
    pair_in, held, far_in, near_in, send, recv,
    small_dp, small_line, partial, small_send, small_recv,
):
    me, dp = lax.axis_index("tensor"), lax.axis_index("dp")
    core, near_x, near_y = [dp + bit * (1 - 2 * ((dp // bit) % 2)) for bit in (1, 2, 4)]
    far = near_x + 4 * (1 - 2 * ((dp // 4) % 2))
    half = grads.shape[1] // 2
    halves = [pl.ds(0, half), pl.ds(half, half)]
    meet(everyone(count, size))
    line = LineScatter(parts, inbox, outbox, line_send, line_recv, count, pieces)
    line.begin()
    order = (far, near_x, near_y, dp)
    pair = [
        remote(
            grads.at[dest + 1 - 2 * (dest % 2)], pair_in.at[k], send.at[k], recv.at[k],
            {"dp": core},
        )
        for k, dest in enumerate(order)
    ]
    for copy in pair:
        copy.start()
    small_copies = [
        remote(small, small_dp.at[k - 1], small_send.at[k - 1], small_recv.at[k - 1],
               {"dp": lax.rem(dp + k, size)})
        for k in range(1, size)
    ]
    for copy in small_copies:
        copy.start()

    def ready(k, which):
        rows = halves[which]
        add_rows(held.at[k, rows], grads.at[order[k], rows], pair_in.at[k, rows], half)

    def flow(slot, src, dst, target):
        return remote(src, dst, send.at[slot], recv.at[slot], {"dp": target})

    pair[0].wait_recv()
    ready(0, 0)
    far_x = flow(4, held.at[0, halves[0]], far_in.at[0], near_x)
    far_x.start()
    ready(0, 1)
    far_y = flow(5, held.at[0, halves[1]], far_in.at[1], near_y)
    far_y.start()
    pair[1].wait_recv()
    ready(1, 0)
    x_low = flow(6, held.at[1, halves[0]], near_in.at[0, halves[0]], near_x)
    x_low.start()
    pair[2].wait_recv()
    ready(2, 1)
    y_high = flow(7, held.at[2, halves[1]], near_in.at[1, halves[1]], near_y)
    y_high.start()
    ready(1, 1)
    ready(2, 0)
    pair[3].wait_recv()
    for copy in small_copies:
        copy.wait_recv()
    gathered = small[...]
    for k in range(size - 1):
        gathered = gathered + small_dp[k]
    partial[...] = gathered
    tiny = [
        remote(partial, small_line.at[k - 1], small_send.at[size - 2 + k],
               small_recv.at[size - 2 + k], {"tensor": lax.rem(me + k, count)})
        for k in range(1, count)
    ]
    for copy in tiny:
        copy.start()
    for piece in range(pieces):
        line.relay(1, piece)
    far_x.wait_recv()
    add_rows(held.at[2, halves[0]], held.at[2, halves[0]], far_in.at[0], half)
    y_low = flow(8, held.at[2, halves[0]], near_in.at[1, halves[0]], near_y)
    y_low.start()
    far_y.wait_recv()
    add_rows(held.at[1, halves[1]], held.at[1, halves[1]], far_in.at[1], half)
    x_high = flow(9, held.at[1, halves[1]], near_in.at[0, halves[1]], near_x)
    x_high.start()
    for time in range(2, count - 1):
        for piece in range(pieces):
            line.relay(time, piece)
    for copy in tiny:
        copy.wait_recv()
    every = partial[...]
    for k in range(count - 1):
        every = every + small_line[k]
    summed[0] = partial[...]
    summed[1] = every
    line.take(total)
    step = 16
    def last(rows_at, near_ready):
        for copy in near_ready:
            copy.wait_recv()
        def body(index, carry):
            at = pl.ds(pl.multiple_of(rows_at + index * step, step), step)
            mine[at, :] = (
                grads[dp, at, :].astype(jnp.float32)
                + pair_in[3, at, :].astype(jnp.float32)
                + near_in[0, at, :].astype(jnp.float32)
                + near_in[1, at, :].astype(jnp.float32)
            )
            return carry
        lax.fori_loop(0, half // step, body, 0)
    last(0, (x_low, y_low))
    last(half, (x_high, y_high))
    for copy in pair + small_copies + tiny + [far_x, far_y, x_low, y_high, y_low, x_high]:
        copy.wait_send()
    line.finish()


def scatter_all(value, grads, small, count, size, pieces=2):
    rows, cols = value.shape[0] // count, value.shape[1]
    block, wide = grads.shape[0] // size, grads.shape[1]
    low = jnp.bfloat16
    return pl.pallas_call(
        functools.partial(scatter_kernel, count, size, pieces),
        out_shape=(
            jax.ShapeDtypeStruct((rows, cols), jnp.float32),
            jax.ShapeDtypeStruct((block, wide), jnp.float32),
            jax.ShapeDtypeStruct((2,) + small.shape, jnp.float32),
        ),
        in_specs=[IN_VMEM] * 3,
        out_specs=(IN_VMEM,) * 3,
        scratch_shapes=line_boxes(count, rows, cols, pieces)
        + [
            pltpu.VMEM((4, block, wide), low),
            pltpu.VMEM((3, block, wide), low),
            pltpu.VMEM((2, block // 2, wide), low),
            pltpu.VMEM((2, block, wide), low),
            pltpu.SemaphoreType.DMA((10,)),
            pltpu.SemaphoreType.DMA((10,)),
            pltpu.VMEM((size - 1,) + small.shape, jnp.float32),
            pltpu.VMEM((count - 1,) + small.shape, jnp.float32),
            pltpu.VMEM(small.shape, jnp.float32),
            pltpu.SemaphoreType.DMA((size + count - 2,)),
            pltpu.SemaphoreType.DMA((size + count - 2,)),
        ],
        compiler_params=pltpu.CompilerParams(
            collective_id=2, has_side_effects=True, vmem_limit_bytes=62 * 1024 * 1024
        ),
        name="scatter_all",
    )(
        value.astype(low).reshape(count, rows, cols),
        grads.astype(low).reshape(size, block, wide),
        small,
    )


def unit_rows(value):
    scale = lax.rsqrt(jnp.mean(value * value, axis=-1, keepdims=True) + EPS)
    return (value * scale, scale)


def unit_back(grad, unit, scale):
    return scale * (grad - unit * jnp.mean(grad * unit, axis=-1, keepdims=True))


def contract_rows(left, right):
    return lax.dot_general(
        left, right, (((0,), (0,)), ((), ())), preferred_element_type=jnp.float32
    )


def contract_cols(left, right):
    return lax.dot_general(
        left, right, (((1,), (1,)), ((), ())), preferred_element_type=jnp.float32
    )


def tables(width, length):
    half_dim = HEAD_DIM // 2
    column = lax.iota(jnp.int32, width)
    within = column % HEAD_DIM
    freq_index = (within % half_dim).astype(jnp.float32)
    frequency = 10000.0 ** (-freq_index / half_dim)
    position = lax.iota(jnp.float32, length)
    angle = position[:, None] * frequency[None, :]
    first_half = (within < half_dim)[None, :]
    heads = width // HEAD_DIM
    member = (
        lax.broadcasted_iota(jnp.int32, (width, heads), 0) // HEAD_DIM
        == lax.broadcasted_iota(jnp.int32, (width, heads), 1)
    ).astype(jnp.float32)
    return (jnp.cos(angle), jnp.sin(angle), first_half, member)


def rope_apply(value, cosine, sine, first_half):
    half_dim = HEAD_DIM // 2
    turned = jnp.where(
        first_half, -jnp.roll(value, -half_dim, axis=1), jnp.roll(value, half_dim, axis=1)
    )
    return value * cosine + turned * sine


def rope_back(grad, cosine, sine, first_half):
    half_dim = HEAD_DIM // 2
    weighted = grad * sine
    turned = jnp.where(
        first_half, jnp.roll(weighted, -half_dim, axis=1), -jnp.roll(weighted, half_dim, axis=1)
    )
    return grad * cosine + turned


def head_unit(value, member):
    mean_sq = (
        jnp.dot(value * value, member, precision=HIGH, preferred_element_type=jnp.float32)
        / HEAD_DIM
    )
    scale = jnp.dot(
        lax.rsqrt(mean_sq + EPS), member.T, precision=HIGH, preferred_element_type=jnp.float32
    )
    return (value * scale, scale)


def head_back(grad, unit, scale, member):
    inner = (
        jnp.dot(grad * unit, member, precision=HIGH, preferred_element_type=jnp.float32) / HEAD_DIM
    )
    spread = jnp.dot(inner, member.T, precision=HIGH, preferred_element_type=jnp.float32)
    return scale * (grad - unit * spread)


def block_scores(query3, key3, start, stop, block):
    scale = HEAD_DIM ** (-0.5)
    scores = (
        jnp.einsum(
            "qhd,khd->hqk", query3[start:stop], key3[:stop], preferred_element_type=jnp.float32
        )
        * scale
    )
    allowed = start + lax.broadcasted_iota(jnp.int32, (block, stop), 0) >= lax.broadcasted_iota(
        jnp.int32, (block, stop), 1
    )
    return jnp.where(allowed[None], scores, -jnp.inf)


def attend(query3, key3, value3, block):
    length = query3.shape[0]
    outputs = []
    totals = []
    for block_id in range(length // block):
        start = block_id * block
        stop = start + block
        scores = block_scores(query3, key3, start, stop, block)
        row_max = jnp.max(scores, axis=-1, keepdims=True)
        log_total = jnp.log(jnp.sum(jnp.exp(scores - row_max), axis=-1, keepdims=True)) + row_max
        weights = jnp.exp(scores - log_total).astype(jnp.bfloat16)
        outputs.append(
            jnp.einsum("hqk,khd->qhd", weights, value3[:stop], preferred_element_type=jnp.float32)
        )
        totals.append(log_total)
    return (jnp.concatenate(outputs, axis=0), totals)


def attend_back(query3, key3, value3, grad3, totals, block):
    length = query3.shape[0]
    scale = HEAD_DIM ** (-0.5)
    query_parts = []
    key_grad = jnp.zeros(key3.shape, jnp.float32)
    value_grad = jnp.zeros(value3.shape, jnp.float32)
    for block_id in range(length // block):
        start = block_id * block
        stop = start + block
        scores = block_scores(query3, key3, start, stop, block)
        probs = jnp.exp(scores - totals[block_id])
        g_probs = jnp.einsum(
            "qhd,khd->hqk", grad3[start:stop], value3[:stop], preferred_element_type=jnp.float32
        )
        inner = jnp.sum(probs * g_probs, axis=-1, keepdims=True)
        g_scores = (probs * (g_probs - inner)).astype(jnp.bfloat16)
        query_parts.append(
            jnp.einsum("hqk,khd->qhd", g_scores, key3[:stop], preferred_element_type=jnp.float32)
            * scale
        )
        key_grad = key_grad.at[:stop].add(
            jnp.einsum(
                "hqk,qhd->khd", g_scores, query3[start:stop], preferred_element_type=jnp.float32
            )
            * scale
        )
        value_grad = value_grad.at[:stop].add(
            jnp.einsum(
                "hqk,qhd->khd",
                probs.astype(jnp.bfloat16),
                grad3[start:stop],
                preferred_element_type=jnp.float32,
            )
        )
    return (jnp.concatenate(query_parts, axis=0), key_grad, value_grad)


def scatter_low(value, axis):
    return lax.psum_scatter(
        value.astype(jnp.bfloat16), axis, scatter_dimension=0, tiled=True
    ).astype(jnp.float32)


def on_device(
    tokens,
    w_query,
    w_key,
    w_value,
    w_out,
    w_up,
    w_gate,
    w_down,
    qk_scale,
    up_scale,
    gate_scale,
    alpha_attn,
    alpha_mlp,
    cotangent,
):
    count, size = lax.axis_size("tensor"), lax.axis_size("dp")
    shard = jnp.concatenate([w_query, w_key, w_value, w_out, w_up, w_gate, w_down], axis=1)
    if size == 8:
        whole, weights = gather_all(tokens, shard, count, size)
        whole = whole.reshape(count * tokens.shape[0], tokens.shape[1])
        weights = weights.reshape(size * shard.shape[0], shard.shape[1])
    else:
        whole = line_gather(tokens, count, 1)
        weights = lax.all_gather(shard, "dp", axis=0, tiled=True)
    heads, units = w_query.shape[1], w_up.shape[1]
    query_w, key_w, value_w, out_w, up_w, gate_w, down_w = jnp.split(
        weights,
        (heads, 2 * heads, 3 * heads, 4 * heads, 4 * heads + units, 4 * heads + 2 * units),
        axis=1,
    )
    length = whole.shape[0]
    width = query_w.shape[1]
    block = min(512, length)
    cosine, sine, first_half, member = tables(width, length)
    shape3 = (length, width // HEAD_DIM, HEAD_DIM)
    q_raw = jnp.dot(whole, query_w, preferred_element_type=jnp.float32)
    k_raw = jnp.dot(whole, key_w, preferred_element_type=jnp.float32)
    value_low = jnp.dot(whole, value_w, preferred_element_type=jnp.float32).astype(jnp.bfloat16)
    q_unit, q_norm = head_unit(rope_apply(q_raw, cosine, sine, first_half), member)
    k_unit, k_norm = head_unit(rope_apply(k_raw, cosine, sine, first_half), member)
    query_low = (q_unit * qk_scale).astype(jnp.bfloat16)
    key_low = (k_unit * qk_scale).astype(jnp.bfloat16)
    query3 = query_low.reshape(shape3)
    key3 = key_low.reshape(shape3)
    value3 = value_low.reshape(shape3)
    attended, totals = attend(query3, key3, value3, block)
    attended_low = attended.reshape(length, width).astype(jnp.bfloat16)
    attn_sum = line_scatter(contract_cols(attended_low, out_w), count, 4)
    attn_unit, attn_norm = unit_rows(attn_sum)
    residual = tokens.astype(jnp.float32)
    mid, mid_norm = unit_rows(residual + alpha_attn * (attn_unit - residual))
    mid_low = mid.astype(jnp.bfloat16)
    mid_whole = line_gather(mid_low, count, 3)
    up_sum = jnp.dot(mid_whole, up_w, preferred_element_type=jnp.float32)
    gate_sum = jnp.dot(mid_whole, gate_w, preferred_element_type=jnp.float32)
    up_val = up_sum * up_scale
    gate_val = gate_sum * gate_scale
    sigma = jax.nn.sigmoid(gate_val)
    hidden_low = (up_val * (gate_val * sigma)).astype(jnp.bfloat16)
    mlp_sum = line_scatter(contract_cols(hidden_low, down_w), count, 7)
    mlp_unit, mlp_norm = unit_rows(mlp_sum)
    final, final_norm = unit_rows(mid + alpha_mlp * (mlp_unit - mid))
    output = final.astype(jnp.bfloat16)
    g_second = unit_back(cotangent.astype(jnp.float32), final, final_norm)
    g_alpha_mlp = jnp.sum((mlp_unit - mid) * g_second, axis=0)
    g_mlp_low = unit_back(alpha_mlp * g_second, mlp_unit, mlp_norm).astype(jnp.bfloat16)
    g_mlp_whole = line_gather(g_mlp_low, count, 5)
    down_grad = contract_rows(g_mlp_whole, hidden_low)
    g_hidden = jnp.dot(g_mlp_whole, down_w, preferred_element_type=jnp.float32)
    g_up = g_hidden * (gate_val * sigma)
    g_gate = g_hidden * up_val * (sigma * (1.0 + gate_val * (1.0 - sigma)))
    up_scale_grad = jnp.sum(g_up * up_sum, axis=0)
    gate_scale_grad = jnp.sum(g_gate * gate_sum, axis=0)
    g_up_low = (g_up * up_scale).astype(jnp.bfloat16)
    g_gate_low = (g_gate * gate_scale).astype(jnp.bfloat16)
    up_grad = contract_rows(mid_whole, g_up_low)
    gate_grad = contract_rows(mid_whole, g_gate_low)
    g_mid_part = contract_cols(g_up_low, up_w) + contract_cols(g_gate_low, gate_w)
    g_mid = (1.0 - alpha_mlp) * g_second + line_scatter(g_mid_part, count, 8)
    g_first = unit_back(g_mid, mid, mid_norm)
    g_alpha_attn = jnp.sum((attn_unit - residual) * g_first, axis=0)
    g_attn_low = unit_back(alpha_attn * g_first, attn_unit, attn_norm).astype(jnp.bfloat16)
    g_attn_whole = line_gather(g_attn_low, count, 6)
    out_grad = contract_rows(g_attn_whole, attended_low)
    g_attended_low = jnp.dot(g_attn_whole, out_w, preferred_element_type=jnp.float32).astype(
        jnp.bfloat16
    )
    g_query3, g_key3, g_value3 = attend_back(
        query3, key3, value3, g_attended_low.reshape(shape3), totals, block
    )
    g_query = g_query3.reshape(length, width)
    g_key = g_key3.reshape(length, width)
    qk_grad = jnp.sum(g_query * q_unit, axis=0) + jnp.sum(g_key * k_unit, axis=0)
    g_q_raw_low = rope_back(
        head_back(g_query * qk_scale, q_unit, q_norm, member), cosine, sine, first_half
    ).astype(jnp.bfloat16)
    g_k_raw_low = rope_back(
        head_back(g_key * qk_scale, k_unit, k_norm, member), cosine, sine, first_half
    ).astype(jnp.bfloat16)
    g_value_low = g_value3.reshape(length, width).astype(jnp.bfloat16)
    query_grad = contract_rows(whole, g_q_raw_low)
    key_grad = contract_rows(whole, g_k_raw_low)
    value_grad = contract_rows(whole, g_value_low)
    g_tok_part = (
        contract_cols(g_q_raw_low, query_w)
        + contract_cols(g_k_raw_low, key_w)
        + contract_cols(g_value_low, value_w)
    )
    grads = jnp.concatenate(
        [query_grad, key_grad, value_grad, out_grad, up_grad, gate_grad, down_grad], axis=1
    )
    model = g_alpha_attn.shape[0]
    vectors = (g_alpha_attn, g_alpha_mlp, up_scale_grad, gate_scale_grad, qk_grad)
    packed = jnp.concatenate(vectors)
    packed = jnp.pad(packed, (0, 8 * model - packed.shape[0])).reshape(8, model)
    if size == 8:
        g_tokens, mine, sums = scatter_all(g_tok_part, grads, packed, count, size)
    else:
        g_tokens = line_scatter(g_tok_part, count, 2)
        mine = scatter_low(grads, "dp")
        within = lax.psum(packed, "dp")
        sums = jnp.stack([within, lax.psum(within, "tensor")])
    tokens_grad = (1.0 - alpha_attn) * g_first + g_tokens
    query_grad, key_grad, value_grad, out_grad, up_grad, gate_grad, down_grad = jnp.split(
        mine,
        (heads, 2 * heads, 3 * heads, 4 * heads, 4 * heads + units, 4 * heads + 2 * units),
        axis=1,
    )
    g_alpha_attn, g_alpha_mlp = sums[1, 0], sums[1, 1]
    flat = sums[0].reshape(8 * model)[2 * model :]
    up_scale_grad, gate_scale_grad = flat[:units], flat[units : 2 * units]
    qk_grad = flat[2 * units : 2 * units + heads]
    return (
        output,
        tokens_grad,
        query_grad,
        key_grad,
        value_grad,
        out_grad,
        up_grad,
        gate_grad,
        down_grad,
        qk_grad,
        up_scale_grad,
        gate_scale_grad,
        g_alpha_attn,
        g_alpha_mlp,
    )


def solution(mesh):
    in_specs = (
        P(("dp", "tensor"), None),
        P("dp", "tensor"),
        P("dp", "tensor"),
        P("dp", "tensor"),
        P("dp", "tensor"),
        P("dp", "tensor"),
        P("dp", "tensor"),
        P("dp", "tensor"),
        P("tensor"),
        P("tensor"),
        P("tensor"),
        P(),
        P(),
        P(("dp", "tensor"), None),
    )
    out_specs = (
        P(("dp", "tensor"), None),
        P(("dp", "tensor"), None),
        P("dp", "tensor"),
        P("dp", "tensor"),
        P("dp", "tensor"),
        P("dp", "tensor"),
        P("dp", "tensor"),
        P("dp", "tensor"),
        P("dp", "tensor"),
        P("tensor"),
        P("tensor"),
        P("tensor"),
        P(),
        P(),
    )
    return jax.shard_map(
        on_device, mesh=mesh, in_specs=in_specs, out_specs=out_specs, check_vma=False
    )
```

```python
import functools

import jax
import jax.numpy as jnp
from jax import lax
from jax.experimental import pallas as pl
from jax.experimental.pallas import tpu as pltpu
from jax.sharding import PartitionSpec as P

HEAD_DIM = 64


HIGH = lax.Precision.HIGHEST
EPS = 1e-06


MESH_ID = pl.DeviceIdType.MESH
ANY = pl.BlockSpec(memory_space=pl.ANY)
IN_VMEM = pl.BlockSpec(memory_space=pltpu.VMEM)


def remote(src, dst, send, recv, target):
    return pltpu.make_async_remote_copy(
        src_ref=src, dst_ref=dst, send_sem=send, recv_sem=recv,
        device_id=target, device_id_type=MESH_ID,
    )


def meet(partners):
    barrier = pltpu.get_barrier_semaphore()
    count = 0
    for there, target in partners:
        if there is True:
            pl.semaphore_signal(barrier, inc=1, device_id=target, device_id_type=MESH_ID)
            count = count + 1
        else:
            @pl.when(there)
            def _():
                pl.semaphore_signal(barrier, inc=1, device_id=target, device_id_type=MESH_ID)
            count = count + there.astype(jnp.int32)
    pl.semaphore_wait(barrier, count)


def line_partners(me, count):
    return [
        (me < count - 1, {"tensor": jnp.minimum(me + 1, count - 1)}),
        (me > 0, {"tensor": jnp.maximum(me - 1, 0)}),
    ]


def plane_partners():
    dp = lax.axis_index("dp")
    return [(True, {"dp": dp + bit * (1 - 2 * ((dp // bit) % 2))}) for bit in (1, 2, 4)]


class LineGather:
    def __init__(self, own, out, send, recv, count, pieces):
        self.own, self.out, self.send, self.recv = own, out, send, recv
        self.count, self.pieces = count, pieces
        self.me = lax.axis_index("tensor")
        self.rows = own.shape[0] // pieces

    def hop(self, way, origin, piece, step):
        target = {"tensor": self.me + way}
        place = self.out.at[origin, pl.ds(piece * self.rows, self.rows)]
        src = self.own.at[pl.ds(piece * self.rows, self.rows)] if step == 0 else place
        side = 0 if way == 1 else 1
        return remote(
            src, place, self.send.at[side, step, piece], self.recv.at[side, step, piece], target
        )

    def can_send(self, way, step):
        near = self.me + way
        origin = self.me - way * step
        return (near >= 0) & (near < self.count) & (origin >= 0) & (origin < self.count)

    def start(self, step, piece):
        for way in (1, -1):
            @pl.when(self.can_send(way, step))
            def _():
                self.hop(way, self.me - way * step, piece, step).start()

    def arrive(self, step, piece):
        for way in (1, -1):
            origin = self.me - way * (step + 1)
            @pl.when((origin >= 0) & (origin < self.count))
            def _():
                place = self.out.at[origin, pl.ds(piece * self.rows, self.rows)]
                side = 0 if way == 1 else 1
                remote(
                    place, place, self.send.at[side, step, piece],
                    self.recv.at[side, step, piece], {"tensor": self.me - way},
                ).wait_recv()

    def finish(self):
        for step in range(self.count - 1):
            for piece in range(self.pieces):
                for way in (1, -1):
                    @pl.when(self.can_send(way, step))
                    def _():
                        self.hop(way, self.me - way * step, piece, step).wait_send()


def gather_kernel(
    count, pieces, tokens, shard, whole, full, line_send, line_recv, send, recv, local
):
    dp = lax.axis_index("dp")
    flip = [dp + bit * (1 - 2 * ((dp // bit) % 2)) for bit in (1, 2, 4)]
    core, near_x, near_y = flip
    far = near_x + 4 * (1 - 2 * ((dp // 4) % 2))
    half = shard.shape[0] // 2
    meet(line_partners(lax.axis_index("tensor"), count) + plane_partners())
    line = LineGather(tokens, whole, line_send, line_recv, count, pieces)

    def part(origin, which):
        return full.at[origin, pl.ds(which * half, half)]

    def flow(slot, src, origin, which, target):
        return remote(src, part(origin, which), send.at[slot], recv.at[slot], {"dp": target})

    mine = [shard.at[pl.ds(which * half, half)] for which in (0, 1)]
    for piece in range(pieces):
        line.start(0, piece)
    started = []

    def go(slot, src, origin, which, target):
        copy = flow(slot, src, origin, which, target)
        copy.start()
        started.append(copy)

    def got(slot, origin, which):
        place = part(origin, which)
        remote(place, place, send.at[slot], recv.at[slot], {"dp": core}).wait_recv()

    go(0, mine[0], dp, 0, near_x)
    go(2, mine[1], dp, 1, near_y)
    go(1, mine[1], dp, 1, near_x)
    go(3, mine[0], dp, 0, near_y)
    go(6, mine[0], dp, 0, core)
    go(7, mine[1], dp, 1, core)
    keep = [
        pltpu.make_async_copy(shard, full.at[dp], local.at[0]),
        pltpu.make_async_copy(tokens, whole.at[line.me], local.at[1]),
    ]
    for copy in keep:
        copy.start()
    for piece in range(pieces):
        line.arrive(0, piece)
        line.start(1, piece)
    got(0, near_x, 0)
    go(4, part(near_x, 0), near_x, 0, near_y)
    go(8, part(near_x, 0), near_x, 0, core)
    got(2, near_y, 1)
    go(5, part(near_y, 1), near_y, 1, near_x)
    go(9, part(near_y, 1), near_y, 1, core)
    for step in range(1, count - 1):
        for piece in range(pieces):
            line.arrive(step, piece)
            if step + 1 < count - 1:
                line.start(step + 1, piece)
    got(1, near_x, 1)
    go(10, part(near_x, 1), near_x, 1, core)
    got(3, near_y, 0)
    go(11, part(near_y, 0), near_y, 0, core)
    got(4, far, 0)
    go(12, part(far, 0), far, 0, core)
    got(5, far, 1)
    go(13, part(far, 1), far, 1, core)
    def other(index):
        return index + 1 - 2 * (index % 2)
    for slot, origin, which in (
        (6, core, 0), (7, core, 1), (8, other(near_x), 0), (9, other(near_y), 1),
        (10, other(near_x), 1), (11, other(near_y), 0), (12, other(far), 0), (13, other(far), 1),
    ):
        got(slot, origin, which)
    for copy in started:
        copy.wait_send()
    line.finish()
    for copy in keep:
        copy.wait()


def gather_all(tokens, shard, count, size, pieces=2):
    return pl.pallas_call(
        functools.partial(gather_kernel, count, pieces),
        out_shape=(
            jax.ShapeDtypeStruct((count,) + tokens.shape, tokens.dtype),
            jax.ShapeDtypeStruct((size,) + shard.shape, shard.dtype),
        ),
        in_specs=[IN_VMEM, IN_VMEM],
        out_specs=(ANY, ANY),
        scratch_shapes=[
            pltpu.SemaphoreType.DMA((2, count - 1, pieces)),
            pltpu.SemaphoreType.DMA((2, count - 1, pieces)),
            pltpu.SemaphoreType.DMA((14,)),
            pltpu.SemaphoreType.DMA((14,)),
            pltpu.SemaphoreType.DMA((2,)),
        ],
        compiler_params=pltpu.CompilerParams(collective_id=1, has_side_effects=True),
        name="gather_all",
    )(tokens, shard)


def everyone(count, size):
    me, dp = lax.axis_index("tensor"), lax.axis_index("dp")
    return [(True, {"tensor": lax.rem(me + k, count)}) for k in range(1, count)] + [
        (True, {"dp": lax.rem(dp + k, size)}) for k in range(1, size)
    ]


def add_rows(dst, left, right, rows):
    step = 16
    def body(index, carry):
        at = pl.ds(pl.multiple_of(index * step, step), step)
        total = left[at, :].astype(jnp.float32) + right[at, :].astype(jnp.float32)
        dst[at, :] = total.astype(dst.dtype)
        return carry
    lax.fori_loop(0, rows // step, body, 0)


class LineScatter:
    def __init__(self, parts, inbox, outbox, send, recv, count, pieces):
        self.parts, self.inbox, self.outbox = parts, inbox, outbox
        self.send, self.recv = send, recv
        self.count, self.pieces = count, pieces
        self.me = lax.axis_index("tensor")
        self.rows = parts.shape[1] // pieces

    def at(self, piece):
        return pl.ds(piece * self.rows, self.rows)

    def copy(self, way, src, dest, piece):
        side = 0 if way == 1 else 1
        return remote(
            src, self.inbox.at[side, dest, self.at(piece)],
            self.send.at[side, dest, piece], self.recv.at[side, dest, piece],
            {"tensor": self.me + way},
        )

    def hops(self, way):
        return self.me if way == 1 else self.count - 1 - self.me

    def begin(self):
        for turn in range(self.count - 1):
            for piece in range(self.pieces):
                for way in (1, -1):
                    dest = self.count - 1 - turn if way == 1 else turn
                    @pl.when(self.hops(way) == 0)
                    def _():
                        self.copy(way, self.parts.at[dest, self.at(piece)], dest, piece).start()

    def relay(self, time, piece):
        for way in (1, -1):
            side = 0 if way == 1 else 1
            turn = time - self.hops(way)
            dest = self.count - 1 - turn if way == 1 else turn
            beyond = dest > self.me if way == 1 else dest < self.me
            @pl.when((self.hops(way) > 0) & (turn >= 0) & beyond)
            def _():
                rows = self.at(piece)
                src = self.outbox.at[side, dest, rows]
                self.copy(way, src, dest, piece).wait_recv()
                add_rows(
                    src, self.parts.at[dest, rows], self.inbox.at[side, dest, rows], self.rows
                )
                self.copy(way, src, dest, piece).start()

    def take(self, total):
        step = 16
        def first(index, carry):
            at = pl.ds(pl.multiple_of(index * step, step), step)
            total[at, :] = self.parts[self.me, at, :].astype(jnp.float32)
            return carry
        lax.fori_loop(0, self.parts.shape[1] // step, first, 0)
        for piece in range(self.pieces):
            for way in (1, -1):
                side = 0 if way == 1 else 1
                @pl.when(self.hops(way) > 0)
                def _():
                    rows = self.at(piece)
                    self.copy(way, self.inbox.at[side, self.me, rows], self.me, piece).wait_recv()
                    add_rows(
                        total.at[rows], total.at[rows], self.inbox.at[side, self.me, rows],
                        self.rows,
                    )

    def finish(self):
        for turn in range(self.count - 1):
            for piece in range(self.pieces):
                for way in (1, -1):
                    dest = self.count - 1 - turn if way == 1 else turn
                    sent = dest > self.me if way == 1 else dest < self.me
                    @pl.when(sent)
                    def _():
                        self.copy(
                            way, self.outbox.at[0 if way == 1 else 1, dest, self.at(piece)],
                            dest, piece,
                        ).wait_send()


def line_boxes(count, rows, cols, pieces):
    return [
        pltpu.VMEM((2, count, rows, cols), jnp.bfloat16),
        pltpu.VMEM((2, count, rows, cols), jnp.bfloat16),
        pltpu.SemaphoreType.DMA((2, count, pieces)),
        pltpu.SemaphoreType.DMA((2, count, pieces)),
    ]


def line_gather_kernel(count, pieces, own, whole, send, recv, local):
    meet(line_partners(lax.axis_index("tensor"), count))
    line = LineGather(own, whole, send, recv, count, pieces)
    for piece in range(pieces):
        line.start(0, piece)
    keep = pltpu.make_async_copy(own, whole.at[line.me], local.at[0])
    keep.start()
    for step in range(count - 1):
        for piece in range(pieces):
            line.arrive(step, piece)
            if step + 1 < count - 1:
                line.start(step + 1, piece)
    line.finish()
    keep.wait()


def line_gather(own, count, ident, pieces=4):
    return pl.pallas_call(
        functools.partial(line_gather_kernel, count, pieces),
        out_shape=jax.ShapeDtypeStruct((count,) + own.shape, own.dtype),
        in_specs=[IN_VMEM],
        out_specs=IN_VMEM,
        scratch_shapes=[
            pltpu.SemaphoreType.DMA((2, count - 1, pieces)),
            pltpu.SemaphoreType.DMA((2, count - 1, pieces)),
            pltpu.SemaphoreType.DMA((1,)),
        ],
        compiler_params=pltpu.CompilerParams(collective_id=ident, has_side_effects=True),
        name=f"line_gather_{ident}",
    )(own).reshape(count * own.shape[0], own.shape[1])


def line_scatter_kernel(count, pieces, parts, total, inbox, outbox, send, recv):
    meet(line_partners(lax.axis_index("tensor"), count))
    line = LineScatter(parts, inbox, outbox, send, recv, count, pieces)
    line.begin()
    for time in range(1, count - 1):
        for piece in range(pieces):
            line.relay(time, piece)
    line.take(total)
    line.finish()


def line_scatter(value, count, ident, pieces=4):
    rows, cols = value.shape[0] // count, value.shape[1]
    return pl.pallas_call(
        functools.partial(line_scatter_kernel, count, pieces),
        out_shape=jax.ShapeDtypeStruct((rows, cols), jnp.float32),
        in_specs=[IN_VMEM],
        out_specs=IN_VMEM,
        scratch_shapes=line_boxes(count, rows, cols, pieces),
        compiler_params=pltpu.CompilerParams(collective_id=ident, has_side_effects=True),
        name=f"line_scatter_{ident}",
    )(value.astype(jnp.bfloat16).reshape(count, rows, cols))


class PlaneScatter:
    def __init__(self, grads, mine, pair_in, held, far_in, near_in, send, recv):
        self.grads, self.mine, self.pair_in, self.held = grads, mine, pair_in, held
        self.far_in, self.near_in, self.send, self.recv = far_in, near_in, send, recv
        dp = lax.axis_index("dp")
        core, near_x, near_y = [dp + bit * (1 - 2 * ((dp // bit) % 2)) for bit in (1, 2, 4)]
        far = near_x + 4 * (1 - 2 * ((dp // 4) % 2))
        self.order = (far, near_x, near_y, dp)
        half = grads.shape[1] // 2
        self.half = half
        low, high = pl.ds(0, half), pl.ds(half, half)
        self.halves = (low, high)
        self.pair = [
            remote(
                grads.at[dest + 1 - 2 * (dest % 2)], pair_in.at[k], send.at[k], recv.at[k],
                {"dp": core},
            )
            for k, dest in enumerate(self.order)
        ]

        def flow(slot, src, dst, target):
            return remote(src, dst, send.at[slot], recv.at[slot], {"dp": target})

        self.far_x = flow(4, held.at[0, low], far_in.at[0], near_x)
        self.far_y = flow(5, held.at[0, high], far_in.at[1], near_y)
        self.x_low = flow(6, held.at[1, low], near_in.at[0, low], near_x)
        self.y_high = flow(7, held.at[2, high], near_in.at[1, high], near_y)
        self.y_low = flow(8, held.at[2, low], near_in.at[1, low], near_y)
        self.x_high = flow(9, held.at[1, high], near_in.at[0, high], near_x)

    def begin(self):
        for copy in self.pair:
            copy.start()

    def ready(self, k, which):
        rows = self.halves[which]
        add_rows(
            self.held.at[k, rows], self.grads.at[self.order[k], rows],
            self.pair_in.at[k, rows], self.half,
        )

    def outward(self):
        self.pair[0].wait_recv()
        self.ready(0, 0)
        self.far_x.start()
        self.ready(0, 1)
        self.far_y.start()
        self.pair[1].wait_recv()
        self.ready(1, 0)
        self.x_low.start()
        self.pair[2].wait_recv()
        self.ready(2, 1)
        self.y_high.start()
        self.ready(1, 1)
        self.ready(2, 0)
        self.pair[3].wait_recv()

    def onward(self):
        low, high = self.halves
        self.far_x.wait_recv()
        add_rows(self.held.at[2, low], self.held.at[2, low], self.far_in.at[0], self.half)
        self.y_low.start()
        self.far_y.wait_recv()
        add_rows(self.held.at[1, high], self.held.at[1, high], self.far_in.at[1], self.half)
        self.x_high.start()

    def take(self):
        step = 16
        for copy in (self.x_low, self.y_low, self.x_high, self.y_high):
            copy.wait_recv()

        def body(index, carry):
            at = pl.ds(pl.multiple_of(index * step, step), step)
            self.mine[at, :] = (
                self.grads[self.order[3], at, :].astype(jnp.float32)
                + self.pair_in[3, at, :].astype(jnp.float32)
                + self.near_in[0, at, :].astype(jnp.float32)
                + self.near_in[1, at, :].astype(jnp.float32)
            )
            return carry

        lax.fori_loop(0, 2 * self.half // step, body, 0)

    def finish(self):
        for copy in self.pair + [
            self.far_x, self.far_y, self.x_low, self.y_high, self.y_low, self.x_high
        ]:
            copy.wait_send()


def plane_boxes(block, wide):
    low = jnp.bfloat16
    return [
        pltpu.VMEM((4, block, wide), low),
        pltpu.VMEM((3, block, wide), low),
        pltpu.VMEM((2, block // 2, wide), low),
        pltpu.VMEM((2, block, wide), low),
        pltpu.SemaphoreType.DMA((10,)),
        pltpu.SemaphoreType.DMA((10,)),
    ]


def blocks(grads, size):
    return grads.astype(jnp.bfloat16).reshape(size, grads.shape[0] // size, grads.shape[1])


def mixed_kernel(
    count, pieces, own, first, second, whole, mine_first, mine_second,
    line_send, line_recv, local, *boxes
):
    meet(line_partners(lax.axis_index("tensor"), count) + plane_partners())
    line = LineGather(own, whole, line_send, line_recv, count, pieces)
    planes = [
        PlaneScatter(first, mine_first, *boxes[:6]),
        PlaneScatter(second, mine_second, *boxes[6:]),
    ]
    for piece in range(pieces):
        line.start(0, piece)
    for plane in planes:
        plane.begin()
    keep = pltpu.make_async_copy(own, whole.at[line.me], local.at[0])
    keep.start()
    planes[0].outward()
    for piece in range(pieces):
        line.arrive(0, piece)
        line.start(1, piece)
    planes[1].outward()
    for piece in range(pieces):
        line.arrive(1, piece)
        line.start(2, piece)
    planes[0].onward()
    planes[1].onward()
    for piece in range(pieces):
        line.arrive(2, piece)
    for plane in planes:
        plane.take()
    for plane in planes:
        plane.finish()
    line.finish()
    keep.wait()


def gather_and_scatter(own, first, second, count, size, pieces=2):
    first, second = blocks(first, size), blocks(second, size)
    whole, mine_first, mine_second = pl.pallas_call(
        functools.partial(mixed_kernel, count, pieces),
        out_shape=(
            jax.ShapeDtypeStruct((count,) + own.shape, own.dtype),
            jax.ShapeDtypeStruct(first.shape[1:], jnp.float32),
            jax.ShapeDtypeStruct(second.shape[1:], jnp.float32),
        ),
        in_specs=[IN_VMEM] * 3,
        out_specs=(IN_VMEM,) * 3,
        scratch_shapes=[
            pltpu.SemaphoreType.DMA((2, count - 1, pieces)),
            pltpu.SemaphoreType.DMA((2, count - 1, pieces)),
            pltpu.SemaphoreType.DMA((1,)),
        ]
        + plane_boxes(*first.shape[1:])
        + plane_boxes(*second.shape[1:]),
        compiler_params=pltpu.CompilerParams(
            collective_id=9, has_side_effects=True, vmem_limit_bytes=60 * 1024 * 1024
        ),
        name="gather_and_scatter",
    )(own, first, second)
    return whole.reshape(count * own.shape[0], own.shape[1]), mine_first, mine_second


def scatter_kernel(
    count, size, pieces, parts, first, second, small, total, mine_first, mine_second, summed,
    inbox, outbox, line_send, line_recv,
    small_dp, small_line, partial, small_send, small_recv, *boxes
):
    me, dp = lax.axis_index("tensor"), lax.axis_index("dp")
    meet(everyone(count, size))
    line = LineScatter(parts, inbox, outbox, line_send, line_recv, count, pieces)
    planes = [
        PlaneScatter(first, mine_first, *boxes[:6]),
        PlaneScatter(second, mine_second, *boxes[6:]),
    ]
    line.begin()
    for plane in planes:
        plane.begin()
    small_copies = [
        remote(small, small_dp.at[k - 1], small_send.at[k - 1], small_recv.at[k - 1],
               {"dp": lax.rem(dp + k, size)})
        for k in range(1, size)
    ]
    for copy in small_copies:
        copy.start()
    for plane in planes:
        plane.outward()
    for copy in small_copies:
        copy.wait_recv()
    gathered = small[...]
    for k in range(size - 1):
        gathered = gathered + small_dp[k]
    partial[...] = gathered
    tiny = [
        remote(partial, small_line.at[k - 1], small_send.at[size - 2 + k],
               small_recv.at[size - 2 + k], {"tensor": lax.rem(me + k, count)})
        for k in range(1, count)
    ]
    for copy in tiny:
        copy.start()
    for piece in range(pieces):
        line.relay(1, piece)
    for plane in planes:
        plane.onward()
    for time in range(2, count - 1):
        for piece in range(pieces):
            line.relay(time, piece)
    for copy in tiny:
        copy.wait_recv()
    every = partial[...]
    for k in range(count - 1):
        every = every + small_line[k]
    summed[0] = partial[...]
    summed[1] = every
    for plane in planes:
        plane.take()
    line.take(total)
    for copy in small_copies + tiny:
        copy.wait_send()
    for plane in planes:
        plane.finish()
    line.finish()


def scatter_all(value, first, second, small, count, size, pieces=4):
    rows, cols = value.shape[0] // count, value.shape[1]
    first, second = blocks(first, size), blocks(second, size)
    return pl.pallas_call(
        functools.partial(scatter_kernel, count, size, pieces),
        out_shape=(
            jax.ShapeDtypeStruct((rows, cols), jnp.float32),
            jax.ShapeDtypeStruct(first.shape[1:], jnp.float32),
            jax.ShapeDtypeStruct(second.shape[1:], jnp.float32),
            jax.ShapeDtypeStruct((2,) + small.shape, jnp.float32),
        ),
        in_specs=[IN_VMEM] * 4,
        out_specs=(IN_VMEM,) * 4,
        scratch_shapes=line_boxes(count, rows, cols, pieces)
        + [
            pltpu.VMEM((size - 1,) + small.shape, jnp.float32),
            pltpu.VMEM((count - 1,) + small.shape, jnp.float32),
            pltpu.VMEM(small.shape, jnp.float32),
            pltpu.SemaphoreType.DMA((size + count - 2,)),
            pltpu.SemaphoreType.DMA((size + count - 2,)),
        ]
        + plane_boxes(*first.shape[1:])
        + plane_boxes(*second.shape[1:]),
        compiler_params=pltpu.CompilerParams(
            collective_id=2, has_side_effects=True, vmem_limit_bytes=60 * 1024 * 1024
        ),
        name="scatter_all",
    )(value.astype(jnp.bfloat16).reshape(count, rows, cols), first, second, small)


def unit_rows(value):
    scale = lax.rsqrt(jnp.mean(value * value, axis=-1, keepdims=True) + EPS)
    return (value * scale, scale)


def unit_back(grad, unit, scale):
    return scale * (grad - unit * jnp.mean(grad * unit, axis=-1, keepdims=True))


def contract_rows(left, right):
    return lax.dot_general(
        left, right, (((0,), (0,)), ((), ())), preferred_element_type=jnp.float32
    )


def contract_cols(left, right):
    return lax.dot_general(
        left, right, (((1,), (1,)), ((), ())), preferred_element_type=jnp.float32
    )


def tables(width, length):
    half_dim = HEAD_DIM // 2
    column = lax.iota(jnp.int32, width)
    within = column % HEAD_DIM
    freq_index = (within % half_dim).astype(jnp.float32)
    frequency = 10000.0 ** (-freq_index / half_dim)
    position = lax.iota(jnp.float32, length)
    angle = position[:, None] * frequency[None, :]
    first_half = (within < half_dim)[None, :]
    heads = width // HEAD_DIM
    member = (
        lax.broadcasted_iota(jnp.int32, (width, heads), 0) // HEAD_DIM
        == lax.broadcasted_iota(jnp.int32, (width, heads), 1)
    ).astype(jnp.float32)
    return (jnp.cos(angle), jnp.sin(angle), first_half, member)


def rope_apply(value, cosine, sine, first_half):
    half_dim = HEAD_DIM // 2
    turned = jnp.where(
        first_half, -jnp.roll(value, -half_dim, axis=1), jnp.roll(value, half_dim, axis=1)
    )
    return value * cosine + turned * sine


def rope_back(grad, cosine, sine, first_half):
    half_dim = HEAD_DIM // 2
    weighted = grad * sine
    turned = jnp.where(
        first_half, jnp.roll(weighted, -half_dim, axis=1), -jnp.roll(weighted, half_dim, axis=1)
    )
    return grad * cosine + turned


def head_unit(value, member):
    mean_sq = (
        jnp.dot(value * value, member, precision=HIGH, preferred_element_type=jnp.float32)
        / HEAD_DIM
    )
    scale = jnp.dot(
        lax.rsqrt(mean_sq + EPS), member.T, precision=HIGH, preferred_element_type=jnp.float32
    )
    return (value * scale, scale)


def head_back(grad, unit, scale, member):
    inner = (
        jnp.dot(grad * unit, member, precision=HIGH, preferred_element_type=jnp.float32) / HEAD_DIM
    )
    spread = jnp.dot(inner, member.T, precision=HIGH, preferred_element_type=jnp.float32)
    return scale * (grad - unit * spread)


def block_scores(query3, key3, start, stop, block):
    scale = HEAD_DIM ** (-0.5)
    scores = (
        jnp.einsum(
            "qhd,khd->hqk", query3[start:stop], key3[:stop], preferred_element_type=jnp.float32
        )
        * scale
    )
    allowed = start + lax.broadcasted_iota(jnp.int32, (block, stop), 0) >= lax.broadcasted_iota(
        jnp.int32, (block, stop), 1
    )
    return jnp.where(allowed[None], scores, -jnp.inf)


def attend(query3, key3, value3, block):
    length = query3.shape[0]
    outputs = []
    totals = []
    for block_id in range(length // block):
        start = block_id * block
        stop = start + block
        scores = block_scores(query3, key3, start, stop, block)
        row_max = jnp.max(scores, axis=-1, keepdims=True)
        log_total = jnp.log(jnp.sum(jnp.exp(scores - row_max), axis=-1, keepdims=True)) + row_max
        weights = jnp.exp(scores - log_total).astype(jnp.bfloat16)
        outputs.append(
            jnp.einsum("hqk,khd->qhd", weights, value3[:stop], preferred_element_type=jnp.float32)
        )
        totals.append(log_total)
    return (jnp.concatenate(outputs, axis=0), totals)


def attend_back(query3, key3, value3, grad3, totals, block):
    length = query3.shape[0]
    scale = HEAD_DIM ** (-0.5)
    query_parts = []
    key_grad = jnp.zeros(key3.shape, jnp.float32)
    value_grad = jnp.zeros(value3.shape, jnp.float32)
    for block_id in range(length // block):
        start = block_id * block
        stop = start + block
        scores = block_scores(query3, key3, start, stop, block)
        probs = jnp.exp(scores - totals[block_id])
        g_probs = jnp.einsum(
            "qhd,khd->hqk", grad3[start:stop], value3[:stop], preferred_element_type=jnp.float32
        )
        inner = jnp.sum(probs * g_probs, axis=-1, keepdims=True)
        g_scores = (probs * (g_probs - inner)).astype(jnp.bfloat16)
        query_parts.append(
            jnp.einsum("hqk,khd->qhd", g_scores, key3[:stop], preferred_element_type=jnp.float32)
            * scale
        )
        key_grad = key_grad.at[:stop].add(
            jnp.einsum(
                "hqk,qhd->khd", g_scores, query3[start:stop], preferred_element_type=jnp.float32
            )
            * scale
        )
        value_grad = value_grad.at[:stop].add(
            jnp.einsum(
                "hqk,qhd->khd",
                probs.astype(jnp.bfloat16),
                grad3[start:stop],
                preferred_element_type=jnp.float32,
            )
        )
    return (jnp.concatenate(query_parts, axis=0), key_grad, value_grad)


def scatter_low(value, axis):
    return lax.psum_scatter(
        value.astype(jnp.bfloat16), axis, scatter_dimension=0, tiled=True
    ).astype(jnp.float32)


def on_device(
    tokens,
    w_query,
    w_key,
    w_value,
    w_out,
    w_up,
    w_gate,
    w_down,
    qk_scale,
    up_scale,
    gate_scale,
    alpha_attn,
    alpha_mlp,
    cotangent,
):
    count, size = lax.axis_size("tensor"), lax.axis_size("dp")
    shard = jnp.concatenate([w_query, w_key, w_value, w_out, w_up, w_gate, w_down], axis=1)
    if size == 8:
        whole, weights = gather_all(tokens, shard, count, size)
        whole = whole.reshape(count * tokens.shape[0], tokens.shape[1])
        weights = weights.reshape(size * shard.shape[0], shard.shape[1])
    else:
        whole = line_gather(tokens, count, 1)
        weights = lax.all_gather(shard, "dp", axis=0, tiled=True)
    heads, units = w_query.shape[1], w_up.shape[1]
    query_w, key_w, value_w, out_w, up_w, gate_w, down_w = jnp.split(
        weights,
        (heads, 2 * heads, 3 * heads, 4 * heads, 4 * heads + units, 4 * heads + 2 * units),
        axis=1,
    )
    length = whole.shape[0]
    width = query_w.shape[1]
    block = min(512, length)
    cosine, sine, first_half, member = tables(width, length)
    shape3 = (length, width // HEAD_DIM, HEAD_DIM)
    q_raw = jnp.dot(whole, query_w, preferred_element_type=jnp.float32)
    k_raw = jnp.dot(whole, key_w, preferred_element_type=jnp.float32)
    value_low = jnp.dot(whole, value_w, preferred_element_type=jnp.float32).astype(jnp.bfloat16)
    q_unit, q_norm = head_unit(rope_apply(q_raw, cosine, sine, first_half), member)
    k_unit, k_norm = head_unit(rope_apply(k_raw, cosine, sine, first_half), member)
    query_low = (q_unit * qk_scale).astype(jnp.bfloat16)
    key_low = (k_unit * qk_scale).astype(jnp.bfloat16)
    query3 = query_low.reshape(shape3)
    key3 = key_low.reshape(shape3)
    value3 = value_low.reshape(shape3)
    attended, totals = attend(query3, key3, value3, block)
    attended_low = attended.reshape(length, width).astype(jnp.bfloat16)
    attn_sum = line_scatter(contract_cols(attended_low, out_w), count, 4)
    attn_unit, attn_norm = unit_rows(attn_sum)
    residual = tokens.astype(jnp.float32)
    mid, mid_norm = unit_rows(residual + alpha_attn * (attn_unit - residual))
    mid_low = mid.astype(jnp.bfloat16)
    mid_whole = line_gather(mid_low, count, 3)
    up_sum = jnp.dot(mid_whole, up_w, preferred_element_type=jnp.float32)
    gate_sum = jnp.dot(mid_whole, gate_w, preferred_element_type=jnp.float32)
    up_val = up_sum * up_scale
    gate_val = gate_sum * gate_scale
    sigma = jax.nn.sigmoid(gate_val)
    hidden_low = (up_val * (gate_val * sigma)).astype(jnp.bfloat16)
    mlp_sum = line_scatter(contract_cols(hidden_low, down_w), count, 7)
    mlp_unit, mlp_norm = unit_rows(mlp_sum)
    final, final_norm = unit_rows(mid + alpha_mlp * (mlp_unit - mid))
    output = final.astype(jnp.bfloat16)
    g_second = unit_back(cotangent.astype(jnp.float32), final, final_norm)
    g_alpha_mlp = jnp.sum((mlp_unit - mid) * g_second, axis=0)
    g_mlp_low = unit_back(alpha_mlp * g_second, mlp_unit, mlp_norm).astype(jnp.bfloat16)
    g_mlp_whole = line_gather(g_mlp_low, count, 5)
    down_grad = contract_rows(g_mlp_whole, hidden_low)
    g_hidden = jnp.dot(g_mlp_whole, down_w, preferred_element_type=jnp.float32)
    g_up = g_hidden * (gate_val * sigma)
    g_gate = g_hidden * up_val * (sigma * (1.0 + gate_val * (1.0 - sigma)))
    up_scale_grad = jnp.sum(g_up * up_sum, axis=0)
    gate_scale_grad = jnp.sum(g_gate * gate_sum, axis=0)
    g_up_low = (g_up * up_scale).astype(jnp.bfloat16)
    g_gate_low = (g_gate * gate_scale).astype(jnp.bfloat16)
    both_grad = contract_rows(mid_whole, jnp.concatenate([g_up_low, g_gate_low], axis=1))
    g_mid_part = contract_cols(g_up_low, up_w) + contract_cols(g_gate_low, gate_w)
    g_mid = (1.0 - alpha_mlp) * g_second + line_scatter(g_mid_part, count, 8)
    g_first = unit_back(g_mid, mid, mid_norm)
    g_alpha_attn = jnp.sum((attn_unit - residual) * g_first, axis=0)
    g_attn_low = unit_back(alpha_attn * g_first, attn_unit, attn_norm).astype(jnp.bfloat16)
    if size == 8:
        g_attn_whole, both_grad, down_grad = gather_and_scatter(
            g_attn_low, both_grad, down_grad, count, size
        )
    else:
        g_attn_whole = line_gather(g_attn_low, count, 6)
        both_grad, down_grad = scatter_low(both_grad, "dp"), scatter_low(down_grad, "dp")
    up_grad, gate_grad = jnp.split(both_grad, 2, axis=1)
    out_grad = contract_rows(g_attn_whole, attended_low)
    g_attended_low = jnp.dot(g_attn_whole, out_w, preferred_element_type=jnp.float32).astype(
        jnp.bfloat16
    )
    g_query3, g_key3, g_value3 = attend_back(
        query3, key3, value3, g_attended_low.reshape(shape3), totals, block
    )
    g_query = g_query3.reshape(length, width)
    g_key = g_key3.reshape(length, width)
    qk_grad = jnp.sum(g_query * q_unit, axis=0) + jnp.sum(g_key * k_unit, axis=0)
    g_q_raw_low = rope_back(
        head_back(g_query * qk_scale, q_unit, q_norm, member), cosine, sine, first_half
    ).astype(jnp.bfloat16)
    g_k_raw_low = rope_back(
        head_back(g_key * qk_scale, k_unit, k_norm, member), cosine, sine, first_half
    ).astype(jnp.bfloat16)
    g_value_low = g_value3.reshape(length, width).astype(jnp.bfloat16)
    triple_grad = contract_rows(
        whole, jnp.concatenate([g_q_raw_low, g_k_raw_low, g_value_low], axis=1)
    )
    g_tok_part = (
        contract_cols(g_q_raw_low, query_w)
        + contract_cols(g_k_raw_low, key_w)
        + contract_cols(g_value_low, value_w)
    )
    model = g_alpha_attn.shape[0]
    vectors = (g_alpha_attn, g_alpha_mlp, up_scale_grad, gate_scale_grad, qk_grad)
    packed = jnp.concatenate(vectors)
    packed = jnp.pad(packed, (0, 8 * model - packed.shape[0])).reshape(8, model)
    if size == 8:
        g_tokens, triple_grad, out_grad, sums = scatter_all(
            g_tok_part, triple_grad, out_grad, packed, count, size
        )
    else:
        g_tokens = line_scatter(g_tok_part, count, 2)
        triple_grad, out_grad = scatter_low(triple_grad, "dp"), scatter_low(out_grad, "dp")
        within = lax.psum(packed, "dp")
        sums = jnp.stack([within, lax.psum(within, "tensor")])
    tokens_grad = (1.0 - alpha_attn) * g_first + g_tokens
    query_grad, key_grad, value_grad = jnp.split(triple_grad, 3, axis=1)
    g_alpha_attn, g_alpha_mlp = sums[1, 0], sums[1, 1]
    flat = sums[0].reshape(8 * model)[2 * model :]
    up_scale_grad, gate_scale_grad = flat[:units], flat[units : 2 * units]
    qk_grad = flat[2 * units : 2 * units + heads]
    return (
        output,
        tokens_grad,
        query_grad,
        key_grad,
        value_grad,
        out_grad,
        up_grad,
        gate_grad,
        down_grad,
        qk_grad,
        up_scale_grad,
        gate_scale_grad,
        g_alpha_attn,
        g_alpha_mlp,
    )


def solution(mesh):
    in_specs = (
        P(("dp", "tensor"), None),
        P("dp", "tensor"),
        P("dp", "tensor"),
        P("dp", "tensor"),
        P("dp", "tensor"),
        P("dp", "tensor"),
        P("dp", "tensor"),
        P("dp", "tensor"),
        P("tensor"),
        P("tensor"),
        P("tensor"),
        P(),
        P(),
        P(("dp", "tensor"), None),
    )
    out_specs = (
        P(("dp", "tensor"), None),
        P(("dp", "tensor"), None),
        P("dp", "tensor"),
        P("dp", "tensor"),
        P("dp", "tensor"),
        P("dp", "tensor"),
        P("dp", "tensor"),
        P("dp", "tensor"),
        P("dp", "tensor"),
        P("tensor"),
        P("tensor"),
        P("tensor"),
        P(),
        P(),
    )
    return jax.shard_map(
        on_device, mesh=mesh, in_specs=in_specs, out_specs=out_specs, check_vma=False
    )
```
